32 devices in a mesh: row: 8 (over z, core), col: 4 (over y, x).
Axes of the slice: x: 2, y: 2, z: 4, core: 2. Of those that a mesh axis runs over, the one named last changes fastest.
Arguments:
- loadings: bfloat16 [8, 32768, 1024], P(None, 'row', 'col'), may hold values from -6 to 6
- weights: bfloat16 [8, 32768, 512], P(None, 'row', 'col'), may hold values from -0.03125 to 0.03125
- specific: float32 [8, 32768], P(None, 'row'), may hold values from 0.2 to 5
- factor_cov: float32 [8, 1024, 1024], P(None, 'col'), may hold values from -0.001953125 to 0.0048828125, as said below
Outputs:
- portfolio_cov: float32 [8, 512, 512], P(None, 'row', 'col')
The draws below stay inside these ranges and needn't reach their ends.
Inputs may be any that keep to these rules, and one draw needn't show every extreme that they name: `factor_cov`: each day's matrix is a symmetric positive definite factor covariance of order 1024.
All inputs are finite; a program needn't handle non-finite values.
Results may differ from the reference program's by a relative error of at most 0.0003.
Values may be sent and summed in bfloat16 or wider, within the bound.
No kernel may reach another device: no remote copies, remote signals or barrier semaphores. Data moves between devices by JAX's collectives and lax.ppermute only.
A program may use at most 128 MiB of HBM per device.

```python
import math
import jax
import jax.numpy as jnp
from jax import lax

N = 32768
R = 1024
K = 512
DAYS = 8


def draw_factor_cov(key, part):
    first_key, second_key = jax.random.split(jax.random.fold_in(key, 11))
    noise = jax.random.normal(first_key, (DAYS, R, R), jnp.float32)
    symmetric = (noise + jnp.swapaxes(noise, 1, 2)) / jnp.sqrt(2.0 * R)
    variances = jax.random.uniform(second_key, (DAYS, R), jnp.float32, 1.0, 3.0)
    identity = jnp.eye(R, dtype=jnp.float32)
    return (identity[None, :, :] * variances[:, :, None] + 0.4 * symmetric) / R


def steps_of(rng, extent, pieces, smallest, largest):
    loudness, own = 1.0, jax.random.fold_in(rng, 6)
    for position, parts in pieces:
        steps = jnp.exp(jax.random.uniform(jax.random.fold_in(own, position), (parts,), jnp.float32, smallest / len(pieces), largest / len(pieces)))
        loudness = loudness * jnp.repeat(steps, extent[position] // parts).reshape([-1 if axis == position else 1 for axis in range(len(extent))])
    return loudness


def normal_values(rng, dims, spread, reach, cuts=(), kind=jnp.bfloat16):
    result = spread * jax.random.normal(rng, dims, jnp.float32)
    if cuts:
        result = result * steps_of(rng, dims, cuts, -0.22, 0.18)
    return jnp.clip(result, -reach, reach).astype(kind)


def setup_inputs(seed: int = 0) -> dict:
    keys = jax.random.split(jax.random.key(seed), 5)
    return {
        "loadings": normal_values(keys[0], (DAYS, N, R), 1.0, 6.0, ((1, 8), (2, 4))),
        "weights": normal_values(keys[1], (DAYS, N, K), N ** -0.5, 0.03125, ((1, 8), (2, 4))),
        "specific": jnp.clip(jnp.exp(math.log(5.0) - 3.218876 * jax.random.uniform(keys[2], (DAYS, N), jnp.float32) ** steps_of(keys[2], (DAYS, N), ((1, 8),), -0.2, 0.2)), 0.2, 5.0),
        "factor_cov": draw_factor_cov(jax.random.fold_in(keys[4], 71), 0),
    }


def one_day(operands):
    loadings, weights, specific, factor_cov = operands
    exposure = jnp.dot(loadings.T, weights, preferred_element_type=jnp.float32)
    weighted = (specific[:, None] * weights.astype(jnp.float32)).astype(jnp.bfloat16)
    specific_cov = jnp.dot(weights.T, weighted, preferred_element_type=jnp.float32)
    left = jnp.dot(exposure.T, factor_cov, precision=lax.Precision.HIGHEST)
    return jnp.dot(left, exposure, precision=lax.Precision.HIGHEST) + specific_cov


def reference(loadings, weights, specific, factor_cov):
    return lax.map(one_day, (loadings, weights, specific, factor_cov))
```

```python
import jax
import jax.numpy as jnp
from jax import lax
from jax.sharding import PartitionSpec as P

HIGH = lax.Precision.HIGHEST


def powers(count):
    return [1 << t for t in range(count.bit_length() - 1)]


def swap(x, axis, bit):
    size = lax.axis_size(axis)
    return lax.ppermute(x, axis, [(i, i ^ bit) for i in range(size)])


def bit_of(index, bit):
    return (index // bit) % 2


def pick(x, where, axis):
    return lax.dynamic_index_in_dim(x, where, axis, keepdims=False)


def contract(left, right):
    return lax.dot_general(left, right, (((0,), (0,)), ((), ())), preferred_element_type=jnp.float32)


def spread(pieces, bits):
    for bit in bits:
        for j in list(pieces):
            pieces[j ^ bit] = swap(pieces[j], "col", bit)
    return jnp.concatenate([pieces[j] for j in sorted(pieces)], axis=1)


def scaled(specific, weights):
    return (specific[:, None] * weights.astype(jnp.float32)).astype(jnp.bfloat16)


def partial_merged(loadings, weights, specific, order):
    bit = order[0]
    mine = bit_of(lax.axis_index("col"), bit)
    halves = [a.reshape((2, a.shape[0] // 2) + a.shape[1:]) for a in (loadings, weights, specific)]
    kept = [pick(a, mine, 0) for a in halves]
    load_in, weight_in = [swap(pick(a, 1 - mine, 0), "col", bit) for a in halves[:2]]
    everyone = spread({0: kept[1], bit: weight_in}, order[1:])
    own = jnp.concatenate([kept[1], weight_in], axis=1)
    right = jnp.concatenate([kept[0], load_in, scaled(kept[2], own)], axis=1)
    return contract(everyone, right)


def partial_static(loadings, weights, specific, order):
    half = loadings.shape[0] // 2
    total = None
    for part, bits in ((slice(0, half), order), (slice(half, None), order[::-1])):
        everyone = spread({0: weights[part]}, bits)
        right = jnp.concatenate([loadings[part], scaled(specific[part], weights[part])], axis=1)
        term = contract(everyone, right)
        total = term if total is None else total + term
    return total


def row_reduce(x):
    rows, cols = lax.axis_size("row"), lax.axis_size("col")
    row, col = lax.axis_index("row"), lax.axis_index("col")
    subs = rows // cols
    days, ports, width = x.shape
    x = x.reshape((days,) + (2,) * (rows.bit_length() - 1) + (ports // rows, width))
    for bit in powers(rows):
        keep = bit_of(row, bit)
        if bit >= subs:
            keep = keep ^ bit_of(col, bit // subs)
        axis = x.ndim - 3
        x = pick(x, keep, axis) + swap(pick(x, 1 - keep, axis), "row", bit)
    return x


def finish(sums, orders, merged, factor_cov):
    rows, cols = lax.axis_size("row"), lax.axis_size("col")
    row, col = lax.axis_index("row"), lax.axis_index("col")
    subs = rows // cols
    factors = factor_cov[0].shape[0]
    own, specific, whole = [], [], []
    for x, order, both in zip(sums, orders, merged):
        if both:
            bit, rest = order[0], order[1:]
            one, two, ports = x[:, :factors], x[:, factors : 2 * factors], (x.shape[1] - 2 * factors) // 2
            there = jnp.concatenate([two, one, x[:, 2 * factors + ports :]], axis=1)
            x = x[:, : 2 * factors + ports] + swap(there, "col", bit)
            blocks = jnp.stack([x[:, :factors], x[:, factors : 2 * factors]])
            names = [0, bit]
            specific.append(x[:, 2 * factors :])
        else:
            rest = order
            blocks, names = x[None, :, :factors], [0]
            specific.append(x[:, factors:])
        own.append(blocks[0])
        for bit in rest:
            blocks = jnp.concatenate([blocks, swap(blocks, "col", bit)])
            names = names + [name ^ bit for name in names]
        blocks = jnp.stack([blocks[names.index(j)] for j in range(cols)])
        whole.append(jnp.concatenate([pick(blocks, col ^ j, 0) for j in range(cols)], axis=1))
    every = jnp.stack(own)
    for bit in powers(rows)[::-1]:
        every = jnp.stack([every, swap(every, "row", bit)], axis=every.ndim - 2)
    every = every.reshape(len(own), -1, factors)
    outs = []
    for t, order in enumerate(orders):
        left = lax.dot_general(whole[t], factor_cov[t], (((1,), (1,)), ((), ())), precision=HIGH)
        part = lax.dot_general(left, every[t], (((1,), (1,)), ((), ())), precision=HIGH)
        lines, ports = part.shape[0], part.shape[1] // cols
        part = jnp.stack([part[:, q * ports : (q + 1) * ports] for q in range(cols)])
        part = part.reshape((2,) * (cols.bit_length() - 1) + (lines, ports))
        left_bits = powers(cols)
        for bit in order:
            keep = bit_of(row // subs, bit) ^ bit_of(col, bit)
            axis = len(left_bits) - 1 - left_bits.index(bit)
            left_bits.remove(bit)
            part = pick(part, keep, axis) + swap(pick(part, 1 - keep, axis), "col", bit)
        part = part.reshape((lines, subs, ports // subs))
        part = jnp.concatenate([pick(part, (row % subs) ^ s, 1) for s in range(subs)], axis=1)
        outs.append(part + specific[t])
    return outs


def groups_of(days, bits):
    order = list(bits)
    late = days - 2
    groups = [[(d, order if d % 2 == 0 else order[::-1], True) for d in range(s, min(s + 2, late))] for s in range(0, late, 2)]
    return groups + [[(d, order, False)] for d in range(max(late, 0), days)]


def shards(loadings, weights, specific, factor_cov):
    results = {}
    for group in groups_of(loadings.shape[0], powers(lax.axis_size("col"))):
        parts = []
        for d, order, both in group:
            build = partial_merged if both else partial_static
            parts.append(build(loadings[d], weights[d], specific[d], order))
        sums = row_reduce(jnp.stack(parts))
        days = [d for d, _, _ in group]
        outs = finish([sums[t] for t in range(len(days))], [g[1] for g in group], [g[2] for g in group], [factor_cov[d] for d in days])
        results.update(zip(days, outs))
    return jnp.stack([results[d] for d in sorted(results)])


def solution(mesh):
    in_specs = (P(None, "row", "col"), P(None, "row", "col"), P(None, "row"), P(None, "col", None))
    out_specs = P(None, "row", "col")
    return jax.shard_map(shards, mesh=mesh, in_specs=in_specs, out_specs=out_specs, check_vma=False)
```
